8 devices in a mesh: hp: 1 (over z), cp: 8 (over y, x, core).
Axes of the slice: x: 2, y: 2, z: 1, core: 2. Of those that a mesh axis runs over, the one named last changes fastest.
Arguments:
- q: bfloat16 [6144, 8, 128], P('cp', 'hp')
- k: bfloat16 [6144, 8, 128], P('cp', 'hp')
- v: bfloat16 [6144, 8, 128], P('cp', 'hp')
- u_bias: float32 [8, 128], P('hp')
- v_bias: float32 [8, 128], P('hp')
- rel_table: bfloat16 [6144, 1024], P('cp')
- w_rel: bfloat16 [1024, 8, 128], P(None, 'hp')
- d_out: bfloat16 [6144, 8, 128], P('cp', 'hp')
Outputs:
- output 1: bfloat16 [6144, 8, 128], P('cp', 'hp')
- output 2: bfloat16 [6144, 8, 128], P('cp', 'hp')
- output 3: bfloat16 [6144, 8, 128], P('cp', 'hp')
- output 4: bfloat16 [6144, 8, 128], P('cp', 'hp')
- output 5: float32 [8, 128], P('hp')
- output 6: float32 [8, 128], P('hp')
- output 7: float32 [1024, 8, 128], P(None, 'hp')
All inputs are finite; a program needn't handle non-finite values.
Results may differ from the reference program's by a relative error of at most 0.0149584.
Values are sent between devices in bfloat16 or wider.
A program may use at most 1 GiB of HBM per device.

```python
import math
import jax
import jax.numpy as jnp
from jax import lax

SEQ_LEN = 6144
HEADS_PART = 8
HEAD_DIM = 128
MODEL_DIM = 1024
ROW_BLOCK = math.gcd(SEQ_LEN, 256)
INV_SQRT = HEAD_DIM ** -0.5


def setup_inputs(seed: int = 0, part: int = 0) -> dict:
    part_key = jax.random.fold_in(jax.random.key(seed), part)
    keys_part = jax.random.split(part_key, 7)
    table_keys = jax.random.split(jax.random.key(seed + 17), 2)
    seq_shape = (SEQ_LEN, HEADS_PART, HEAD_DIM)
    head_shape = (HEADS_PART, HEAD_DIM)
    q = jax.random.normal(keys_part[0], seq_shape, jnp.float32)
    k = 2.0 * jax.random.normal(keys_part[1], seq_shape, jnp.float32)
    v = jax.random.normal(keys_part[2], seq_shape, jnp.float32)
    u_bias = 0.5 * jax.random.normal(keys_part[3], head_shape, jnp.float32)
    v_bias = jax.random.normal(keys_part[4], head_shape, jnp.float32)
    w_rel = jax.random.normal(keys_part[5], (MODEL_DIM, HEADS_PART, HEAD_DIM), jnp.float32) * MODEL_DIM ** -0.5
    d_out = jax.random.normal(keys_part[6], seq_shape, jnp.float32)
    freq_cols = 10000.0 ** (-jax.random.uniform(table_keys[0], (MODEL_DIM,), jnp.float32))
    phases = 2.0 * math.pi * jax.random.uniform(table_keys[1], (MODEL_DIM,), jnp.float32)
    offsets = jnp.arange(SEQ_LEN, dtype=jnp.float32)
    rel_table = jnp.sin(offsets[:, None] * freq_cols[None, :] + phases[None, :])
    return {
        'q': q.astype(jnp.bfloat16),
        'k': k.astype(jnp.bfloat16),
        'v': v.astype(jnp.bfloat16),
        'u_bias': u_bias,
        'v_bias': v_bias,
        'rel_table': rel_table.astype(jnp.bfloat16),
        'w_rel': w_rel.astype(jnp.bfloat16),
        'd_out': d_out.astype(jnp.bfloat16),
    }


def attention(q_u, q_v, k, v, rel):
    key_pos = jnp.arange(SEQ_LEN)

    def one_head(head_args):
        qu_h, qv_h, k_h, v_h, rel_h = head_args

        def row_block(start):
            qu_rows = lax.dynamic_slice_in_dim(qu_h, start, ROW_BLOCK)
            qv_rows = lax.dynamic_slice_in_dim(qv_h, start, ROW_BLOCK)
            query_pos = start + jnp.arange(ROW_BLOCK)
            offset_ij = query_pos[:, None] - key_pos[None, :]
            content = jnp.dot(qu_rows, k_h.T)
            by_offset = jnp.dot(qv_rows, rel_h.T)
            position = jnp.take_along_axis(by_offset, jnp.clip(offset_ij, 0, SEQ_LEN - 1), axis=1)
            score_ij = jnp.where(offset_ij >= 0, (content + position) * INV_SQRT, -jnp.inf)
            return jnp.dot(jax.nn.softmax(score_ij, axis=-1), v_h)

        starts = jnp.arange(0, SEQ_LEN, ROW_BLOCK)
        return lax.map(jax.checkpoint(row_block), starts).reshape(SEQ_LEN, HEAD_DIM)

    per_head = lax.map(jax.checkpoint(one_head), tuple(stacked.transpose(1, 0, 2) for stacked in (q_u, q_v, k, v, rel)))
    return per_head.transpose(1, 0, 2)


def reference(q, k, v, u_bias, v_bias, rel_table, w_rel, d_out):
    rel = jnp.dot(rel_table, w_rel.reshape(MODEL_DIM, HEADS_PART * HEAD_DIM), preferred_element_type=jnp.float32)
    rel = rel.astype(jnp.bfloat16).reshape(SEQ_LEN, HEADS_PART, HEAD_DIM)
    q_wide = q.astype(jnp.float32)
    q_u = (q_wide + u_bias).astype(jnp.bfloat16).astype(jnp.float32)
    q_v = (q_wide + v_bias).astype(jnp.bfloat16).astype(jnp.float32)
    out_full, pullback = jax.vjp(attention, q_u, q_v, k.astype(jnp.float32), v.astype(jnp.float32), rel.astype(jnp.float32))
    g_qu, g_qv, g_k, g_v, g_rel = pullback(d_out.astype(jnp.float32))
    d_rel = g_rel.astype(jnp.bfloat16).reshape(SEQ_LEN, HEADS_PART * HEAD_DIM)
    d_w_rel = jnp.dot(rel_table.T, d_rel, preferred_element_type=jnp.float32).reshape(MODEL_DIM, HEADS_PART, HEAD_DIM)
    return (
        out_full.astype(jnp.bfloat16),
        (g_qu + g_qv).astype(jnp.bfloat16),
        g_k.astype(jnp.bfloat16),
        g_v.astype(jnp.bfloat16),
        g_qu.sum(axis=0),
        g_qv.sum(axis=0),
        d_w_rel,
    )
```

```python
import functools
import jax
import jax.numpy as jnp
from jax import lax
from jax.experimental import pallas as pl
from jax.experimental.pallas import tpu as pltpu
from jax.sharding import PartitionSpec as P

TILE = 256
BLK = 128
LOG2E = 1.4426950408889634


def dot_nt(lhs, rhs):
    return lax.dot_general(lhs, rhs, (((1,), (1,)), ((), ())), preferred_element_type=jnp.float32)


def dot_nn(lhs, rhs):
    return lax.dot_general(lhs, rhs, (((1,), (0,)), ((), ())), preferred_element_type=jnp.float32)


def head_kernel(x_hbm, u_ref, w_ref, y_ref, sums_ref,
                q_s, k_s, v_s, g_s, r_s, score_s, roll_s, ds_s, out_s, gu_s, gv_s, max_s, sum_s,
                qv_s, qu_s, quT_s, qvT_s, gT_s, dk_s, dv_s, dr_s, in_sem):
    n_src, _, rows, dim = x_hbm.shape
    n_tiles = n_src * rows // TILE
    nb = TILE // BLK
    inv_sqrt = dim ** -0.5
    scale2 = inv_sqrt * LOG2E
    bf16 = jnp.bfloat16
    f32 = jnp.float32

    copies = []
    for src in range(n_src):
        for arr, dst in enumerate((q_s, k_s, v_s, g_s, r_s)):
            copies.append(pltpu.make_async_copy(x_hbm.at[src, arr], dst.at[pl.ds(src * rows, rows)], in_sem.at[src, arr]))
    for copy in copies:
        copy.start()
    for copy in copies:
        copy.wait()

    sums_ref[...] = jnp.zeros_like(sums_ref)
    dk_s[...] = jnp.zeros_like(dk_s)
    dv_s[...] = jnp.zeros_like(dv_s)
    dr_s[...] = jnp.zeros_like(dr_s)

    row_id = lax.broadcasted_iota(jnp.int32, (BLK, BLK), 0)
    col_id = lax.broadcasted_iota(jnp.int32, (BLK, BLK), 1)
    low = col_id <= row_id

    def tile_rows(ref, idx):
        return ref[pl.ds(pl.multiple_of(idx * TILE, TILE), TILE), :]

    def blk(ref, slot, h, u):
        return ref[slot, pl.ds(h * BLK, BLK), pl.ds(u * BLK, BLK)]

    def by_off(ref, cur, prev, h, d):
        return blk(ref, cur, h, d) if d >= 0 else blk(ref, prev, h, d + nb)

    back_idx = lax.rem(col_id + row_id + 1, BLK)

    def unroll_blk(x):
        return jnp.take_along_axis(x, back_idx, axis=1)

    @pl.loop(0, n_tiles)
    def _(i):
        q_wide = tile_rows(q_s, i).astype(f32)
        qu_f = q_wide + u_ref[...]
        qv_f = q_wide + w_ref[...]
        qu_s[...] = qu_f.astype(bf16)
        qv_s[...] = qv_f.astype(bf16)
        quT_s[...] = qu_f.T.astype(bf16)
        qvT_s[...] = qv_f.T.astype(bf16)
        g_tile = tile_rows(g_s, i)
        gT_s[...] = g_tile.astype(f32).T.astype(bf16)
        max_s[...] = jnp.full_like(max_s, -jnp.inf)
        sum_s[...] = jnp.zeros_like(sum_s)
        out_s[...] = jnp.zeros_like(out_s)
        gu_s[...] = jnp.zeros_like(gu_s)
        gv_s[...] = jnp.zeros_like(gv_s)

        def score_step(m, diag):
            kt = i - m
            cur = lax.rem(m, 2)
            prev = 1 - cur
            by_offset = dot_nt(qv_s[...], tile_rows(r_s, m))
            for h in range(nb):
                for d in range(nb):
                    piece = by_offset[h * BLK:(h + 1) * BLK, d * BLK:(d + 1) * BLK]
                    roll_s[cur, pl.ds(h * BLK, BLK), pl.ds(d * BLK, BLK)] = pltpu.roll(piece, 1, 1, stride=1, stride_axis=0)
            content = dot_nt(qu_s[...], tile_rows(k_s, kt))
            for h in range(nb):
                top = max_s[pl.ds(h * BLK, BLK), :]
                for u in range(nb):
                    piece = content[h * BLK:(h + 1) * BLK, u * BLK:(u + 1) * BLK]
                    if diag and u > h:
                        s_blk = jnp.full((BLK, BLK), -jnp.inf, f32)
                    elif diag and u == h:
                        s_blk = jnp.where(low, piece + by_off(roll_s, cur, prev, h, 0), -jnp.inf)
                    else:
                        s_blk = piece + jnp.where(low, by_off(roll_s, cur, prev, h, h - u), by_off(roll_s, cur, prev, h, h - u - 1))
                    score_s[kt, pl.ds(h * BLK, BLK), pl.ds(u * BLK, BLK)] = s_blk
                    top = jnp.maximum(top, s_blk)
                max_s[pl.ds(h * BLK, BLK), :] = top

        score_step(0, True)

        @pl.loop(1, i + 1)
        def _(m):
            score_step(m, False)

        row_max = jnp.max(max_s[...], axis=1, keepdims=True) * scale2

        @pl.loop(0, i + 1)
        def _(kt):
            prob = jnp.exp2(score_s[kt] * scale2 - row_max)
            score_s[kt] = prob
            part = prob[:, :BLK]
            for u in range(1, nb):
                part = part + prob[:, u * BLK:(u + 1) * BLK]
            sum_s[...] += part
            out_s[...] += dot_nn(prob.astype(bf16), tile_rows(v_s, kt))

        inv_sum = 1.0 / jnp.sum(sum_s[...], axis=1, keepdims=True)
        out = out_s[...] * inv_sum
        delta = jnp.sum(out * g_tile.astype(f32), axis=1, keepdims=True)
        per = rows // TILE
        c_idx = i // per
        r_idx = pl.multiple_of(lax.rem(i, per) * TILE, TILE)
        y_ref[c_idx, 0, pl.ds(r_idx, TILE), :] = out.astype(bf16)
        ds_s[1] = jnp.zeros((TILE, TILE), f32)

        @pl.loop(0, i + 1)
        def _(kt):
            m = i - kt
            cur = lax.rem(kt, 2)
            prev = 1 - cur
            d_prob = dot_nt(tile_rows(g_s, i), tile_rows(v_s, kt))
            prob = score_s[kt] * inv_sum
            d_score = prob * (d_prob - delta)
            ds_s[cur] = d_score
            prob_b = prob.astype(bf16)
            ds_b = d_score.astype(bf16)
            dv_s[kt] += dot_nn(gT_s[...], prob_b)
            dk_s[kt] += dot_nn(quT_s[...], ds_b)
            gu_s[...] += dot_nn(ds_b, tile_rows(k_s, kt))
            out_rows = []
            for h in range(nb):
                cols = []
                for d in range(nb):
                    near = by_off(ds_s, cur, prev, h, h - d)
                    far = by_off(ds_s, cur, prev, h, h - d - 1)
                    cols.append(unroll_blk(jnp.where(low, near, far)))
                out_rows.append(jnp.concatenate(cols, axis=1))
            wide = jnp.concatenate(out_rows, axis=0).astype(bf16)
            gv_s[...] += dot_nn(wide, tile_rows(r_s, m))
            dr_s[m] += dot_nn(qvT_s[...], wide)

        gu = gu_s[...] * inv_sqrt
        gv = gv_s[...] * inv_sqrt
        y_ref[c_idx, 1, pl.ds(r_idx, TILE), :] = (gu + gv).astype(bf16)
        sums_ref[0:1, :] += jnp.sum(gu, axis=0, keepdims=True)
        sums_ref[1:2, :] += jnp.sum(gv, axis=0, keepdims=True)

    @pl.loop(0, n_tiles)
    def _(t):
        per = rows // TILE
        c_idx = t // per
        r_idx = pl.multiple_of(lax.rem(t, per) * TILE, TILE)
        y_ref[c_idx, 2, pl.ds(r_idx, TILE), :] = (dk_s[t] * inv_sqrt).T.astype(bf16)
        y_ref[c_idx, 3, pl.ds(r_idx, TILE), :] = dv_s[t].T.astype(bf16)
        y_ref[c_idx, 4, pl.ds(r_idx, TILE), :] = (dr_s[t] * inv_sqrt).T.astype(bf16)


def run_head(x, u_row, v_row):
    n_src, n_arr, rows, dim = x.shape
    seq = n_src * rows
    n_tiles = seq // TILE
    bf16 = jnp.bfloat16
    f32 = jnp.float32
    vmem = pl.BlockSpec(memory_space=pltpu.VMEM)
    tall = pltpu.VMEM((seq, dim), bf16)
    return pl.pallas_call(
        head_kernel,
        out_shape=(jax.ShapeDtypeStruct((n_src, n_arr, rows, dim), bf16), jax.ShapeDtypeStruct((8, dim), f32)),
        in_specs=[pl.BlockSpec(memory_space=pl.ANY), vmem, vmem],
        out_specs=(vmem, vmem),
        scratch_shapes=[
            tall, tall, tall, tall, tall,
            pltpu.VMEM((n_tiles, TILE, TILE), f32),
            pltpu.VMEM((2, TILE, TILE), f32),
            pltpu.VMEM((2, TILE, TILE), f32),
            pltpu.VMEM((TILE, dim), f32),
            pltpu.VMEM((TILE, dim), f32),
            pltpu.VMEM((TILE, dim), f32),
            pltpu.VMEM((TILE, BLK), f32),
            pltpu.VMEM((TILE, BLK), f32),
            pltpu.VMEM((TILE, dim), bf16),
            pltpu.VMEM((TILE, dim), bf16),
            pltpu.VMEM((dim, TILE), bf16),
            pltpu.VMEM((dim, TILE), bf16),
            pltpu.VMEM((dim, TILE), bf16),
            pltpu.VMEM((n_tiles, dim, TILE), f32),
            pltpu.VMEM((n_tiles, dim, TILE), f32),
            pltpu.VMEM((n_tiles, dim, TILE), f32),
            pltpu.SemaphoreType.DMA((n_src, n_arr)),
        ],
        compiler_params=pltpu.CompilerParams(vmem_limit_bytes=60 * 1024 * 1024),
        cost_estimate=pl.CostEstimate(flops=9 * seq * seq * dim, bytes_accessed=4 * seq * n_arr * dim, transcendentals=seq * seq // 2),
        name='rel_attention_head',
    )(x, u_row, v_row)


def solution(mesh):
    seq_spec = P('cp', 'hp', None)
    head_spec = P('hp', None)
    weight_spec = P(None, 'hp', None)

    def local_fn(q, k, v, u_bias, v_bias, rel_table, w_rel, d_out):
        block_len, num_heads, head_dim = q.shape
        model_dim = rel_table.shape[1]
        f32 = jnp.float32
        bf16 = jnp.bfloat16
        me = lax.axis_index('cp')
        flipped = rel_table.reshape(block_len // BLK, BLK, model_dim)[:, ::-1].reshape(block_len, model_dim)
        table_all = lax.all_gather(flipped, 'cp', axis=0, tiled=True)
        rel_mine = jnp.dot(flipped, w_rel.reshape(model_dim, num_heads * head_dim), preferred_element_type=f32)
        rel_mine = rel_mine.astype(bf16).reshape(block_len, num_heads, head_dim)
        packed = jnp.stack([q, k, v, d_out, rel_mine], axis=0).transpose(2, 0, 1, 3)
        arrived = lax.all_to_all(packed, 'cp', 0, 0, tiled=True)
        u_row = lax.dynamic_slice_in_dim(u_bias, me, 1, 0)
        v_row = lax.dynamic_slice_in_dim(v_bias, me, 1, 0)
        y, sums = run_head(arrived, u_row, v_row)
        d_rel = y[:, 4].reshape(-1, head_dim)
        back = lax.all_to_all(y[:, :4], 'cp', 0, 0, tiled=True)
        back = back.transpose(1, 2, 0, 3)
        d_w = lax.dot_general(table_all, d_rel, (((0,), (0,)), ((), ())), preferred_element_type=f32)
        tail = lax.all_gather(jnp.concatenate([d_w, sums], axis=0), 'cp')
        d_w_rel = tail[:, :model_dim].transpose(1, 0, 2)
        return back[0], back[1], back[2], back[3], tail[:, model_dim], tail[:, model_dim + 1], d_w_rel

    return jax.shard_map(
        local_fn,
        mesh=mesh,
        in_specs=(seq_spec, seq_spec, seq_spec, head_spec, head_spec, P('cp', None), weight_spec, seq_spec),
        out_specs=(seq_spec, seq_spec, seq_spec, seq_spec, head_spec, head_spec, weight_spec),
        check_vma=False,
    )
```

```python
import functools
import jax
import jax.numpy as jnp
from jax import lax
from jax.experimental import pallas as pl
from jax.experimental.pallas import tpu as pltpu
from jax.sharding import PartitionSpec as P

TILE = 768
BLK = 128
LOG2E = 1.4426950408889634


def dot_nt(lhs, rhs):
    return lax.dot_general(lhs, rhs, (((1,), (1,)), ((), ())), preferred_element_type=jnp.float32)


def dot_nn(lhs, rhs):
    return lax.dot_general(lhs, rhs, (((1,), (0,)), ((), ())), preferred_element_type=jnp.float32)


def head_kernel(x_hbm, u_ref, w_ref, y_hbm, drel_ref, sums_ref,
                q_s, k_s, v_s, g_s, r_s, score_s, roll_s, ds_s, out_s, gu_s, gv_s, max_s, sum_s,
                qv_s, qu_s, quT_s, qvT_s, gT_s, dk_s, dv_s, dr_s, stage_s,
                in_send, in_recv, out_send, out_recv):
    n_src, _, rows, dim = x_hbm.shape
    n_tiles = n_src * rows // TILE
    nb = TILE // BLK
    inv_sqrt = dim ** -0.5
    scale2 = inv_sqrt * LOG2E
    bf16 = jnp.bfloat16
    f32 = jnp.float32

    me = lax.axis_index('cp')
    n_dev = n_src
    arrays = (q_s, k_s, v_s, g_s, r_s)

    def arrive(arr, src):
        rows_of = arrays[arr].at[pl.ds(pl.multiple_of(src * rows, rows), rows)]
        return pltpu.make_async_copy(x_hbm.at[me, arr], rows_of, in_recv.at[arr, src])

    def depart(arr, dest):
        return pltpu.make_async_remote_copy(
            src_ref=x_hbm.at[dest, arr],
            dst_ref=arrays[arr].at[pl.ds(pl.multiple_of(me * rows, rows), rows)],
            send_sem=in_send.at[arr, dest], recv_sem=in_recv.at[arr, me],
            device_id={'cp': dest}, device_id_type=pl.DeviceIdType.MESH)

    def give(arr, dest):
        return pltpu.make_async_remote_copy(
            src_ref=stage_s.at[arr, dest], dst_ref=y_hbm.at[me, arr],
            send_sem=out_send.at[arr, dest], recv_sem=out_recv.at[arr, me],
            device_id={'cp': dest}, device_id_type=pl.DeviceIdType.MESH)

    def keep(arr, src):
        return pltpu.make_async_copy(stage_s.at[arr, me], y_hbm.at[src, arr], out_recv.at[arr, src])

    def hand_out(arr, dest):
        @pl.when(dest != me)
        def _():
            give(arr, dest).start()

        @pl.when(dest == me)
        def _():
            keep(arr, me).start()

    barrier = pltpu.get_barrier_semaphore()
    for step in range(1, n_dev):
        pl.semaphore_signal(barrier, inc=1, device_id={'cp': lax.rem(me + step, n_dev)}, device_id_type=pl.DeviceIdType.MESH)
    pl.semaphore_wait(barrier, n_dev - 1)
    order = (1, 0, 4, 2, 3)
    for arr in order:
        for step in range(1, n_dev):
            depart(arr, lax.rem(me + step, n_dev)).start()
        arrive(arr, me).start()

    sums_ref[...] = jnp.zeros_like(sums_ref)
    dk_s[...] = jnp.zeros_like(dk_s)
    dv_s[...] = jnp.zeros_like(dv_s)
    dr_s[...] = jnp.zeros_like(dr_s)

    row_id = lax.broadcasted_iota(jnp.int32, (BLK, BLK), 0)
    col_id = lax.broadcasted_iota(jnp.int32, (BLK, BLK), 1)
    low = col_id <= row_id

    def tile_rows(ref, idx):
        return ref[pl.ds(pl.multiple_of(idx * TILE, TILE), TILE), :]

    def blk(ref, slot, h, u):
        return ref[slot, pl.ds(h * BLK, BLK), pl.ds(u * BLK, BLK)]

    def by_off(ref, cur, prev, h, d):
        return blk(ref, cur, h, d) if d >= 0 else blk(ref, prev, h, d + nb)

    flip = jnp.where(row_id + col_id == BLK - 1, 1.0, 0.0).astype(bf16)

    back_idx = lax.rem(col_id + row_id + 1, BLK)

    def unroll_blk(x):
        return jnp.take_along_axis(x, back_idx, axis=1)

    @pl.loop(0, n_tiles)
    def _(i):
        for arr in order[:3]:
            arrive(arr, i).wait()
        for b in range(nb):
            here = pl.ds(pl.multiple_of(i * TILE + b * BLK, BLK), BLK)
            r_s[here, :] = dot_nn(flip, r_s[here, :]).astype(bf16)
        q_wide = tile_rows(q_s, i).astype(f32)
        qu_f = q_wide + u_ref[...]
        qv_f = q_wide + w_ref[...]
        qu_s[...] = qu_f.astype(bf16)
        qv_s[...] = qv_f.astype(bf16)
        quT_s[...] = qu_f.T.astype(bf16)
        qvT_s[...] = qv_f.T.astype(bf16)
        max_s[...] = jnp.full_like(max_s, -jnp.inf)
        sum_s[...] = jnp.zeros_like(sum_s)
        out_s[...] = jnp.zeros_like(out_s)
        gu_s[...] = jnp.zeros_like(gu_s)
        gv_s[...] = jnp.zeros_like(gv_s)

        def score_step(m, diag):
            kt = i - m
            cur = lax.rem(m, 2)
            prev = 1 - cur
            by_offset = dot_nt(qv_s[...], tile_rows(r_s, m))
            for h in range(nb):
                for d in range(nb):
                    piece = by_offset[h * BLK:(h + 1) * BLK, d * BLK:(d + 1) * BLK]
                    roll_s[cur, pl.ds(h * BLK, BLK), pl.ds(d * BLK, BLK)] = pltpu.roll(piece, 1, 1, stride=1, stride_axis=0)
            content = dot_nt(qu_s[...], tile_rows(k_s, kt))
            for h in range(nb):
                top = max_s[pl.ds(h * BLK, BLK), :]
                for u in range(nb):
                    piece = content[h * BLK:(h + 1) * BLK, u * BLK:(u + 1) * BLK]
                    if diag and u > h:
                        s_blk = jnp.full((BLK, BLK), -jnp.inf, f32)
                    elif diag and u == h:
                        s_blk = jnp.where(low, piece + by_off(roll_s, cur, prev, h, 0), -jnp.inf)
                    else:
                        s_blk = piece + jnp.where(low, by_off(roll_s, cur, prev, h, h - u), by_off(roll_s, cur, prev, h, h - u - 1))
                    score_s[kt, pl.ds(h * BLK, BLK), pl.ds(u * BLK, BLK)] = s_blk
                    top = jnp.maximum(top, s_blk)
                max_s[pl.ds(h * BLK, BLK), :] = top

        score_step(0, True)

        @pl.loop(1, i + 1)
        def _(m):
            score_step(m, False)

        arrive(2, i).wait()
        row_max = jnp.max(max_s[...], axis=1, keepdims=True) * scale2

        @pl.loop(0, i + 1)
        def _(kt):
            prob = jnp.exp2(score_s[kt] * scale2 - row_max)
            score_s[kt] = prob
            part = prob[:, :BLK]
            for u in range(1, nb):
                part = part + prob[:, u * BLK:(u + 1) * BLK]
            sum_s[...] += part
            out_s[...] += dot_nn(prob.astype(bf16), tile_rows(v_s, kt))

        arrive(3, i).wait()
        g_tile = tile_rows(g_s, i)
        gT_s[...] = g_tile.astype(f32).T.astype(bf16)
        inv_sum = 1.0 / jnp.sum(sum_s[...], axis=1, keepdims=True)
        out = out_s[...] * inv_sum
        delta = jnp.sum(out * g_tile.astype(f32), axis=1, keepdims=True)
        stage_s[0, i] = out.astype(bf16)

        @pl.when(i > 0)
        def _():
            hand_out(1, i - 1)

        ds_s[1] = jnp.zeros((TILE, TILE), f32)

        @pl.loop(0, i + 1)
        def _(kt):
            m = i - kt
            cur = lax.rem(kt, 2)
            prev = 1 - cur
            d_prob = dot_nt(tile_rows(g_s, i), tile_rows(v_s, kt))
            prob = score_s[kt] * inv_sum
            d_score = prob * (d_prob - delta)
            ds_s[cur] = d_score
            prob_b = prob.astype(bf16)
            ds_b = d_score.astype(bf16)
            dv_s[kt] += dot_nn(gT_s[...], prob_b)
            dk_s[kt] += dot_nn(quT_s[...], ds_b)
            gu_s[...] += dot_nn(ds_b, tile_rows(k_s, kt))
            out_rows = []
            for h in range(nb):
                cols = []
                for d in range(nb):
                    near = by_off(ds_s, cur, prev, h, h - d)
                    far = by_off(ds_s, cur, prev, h, h - d - 1)
                    cols.append(unroll_blk(jnp.where(low, near, far)))
                out_rows.append(jnp.concatenate(cols, axis=1))
            wide = jnp.concatenate(out_rows, axis=0).astype(bf16)
            gv_s[...] += dot_nn(wide, tile_rows(r_s, m))
            dr_s[m] += dot_nn(qvT_s[...], wide)

            @pl.when(i == n_tiles - 1)
            def _():
                stage_s[2, kt] = (dk_s[kt] * inv_sqrt).T.astype(bf16)
                stage_s[3, kt] = dv_s[kt].T.astype(bf16)

                @pl.when(kt > 0)
                def _():
                    hand_out(2, kt - 1)
                    hand_out(3, kt - 1)

        hand_out(0, i)
        gu = gu_s[...] * inv_sqrt
        gv = gv_s[...] * inv_sqrt
        stage_s[1, i] = (gu + gv).astype(bf16)
        sums_ref[0:1, :] += jnp.sum(gu, axis=0, keepdims=True)
        sums_ref[1:2, :] += jnp.sum(gv, axis=0, keepdims=True)

    hand_out(2, n_tiles - 1)
    hand_out(3, n_tiles - 1)
    for t in range(n_tiles):
        d_rel = (dr_s[t] * inv_sqrt).T.astype(bf16)
        for b in range(nb):
            drel_ref[pl.ds(t * TILE + b * BLK, BLK), :] = dot_nn(flip, d_rel[b * BLK:(b + 1) * BLK]).astype(bf16)
    hand_out(1, n_tiles - 1)
    for step in range(1, n_dev):
        dest = lax.rem(me + step, n_dev)
        for arr in range(5):
            depart(arr, dest).wait_send()
        for arr in range(4):
            give(arr, dest).wait_send()
    for src in range(n_dev):
        for arr in range(4):
            keep(arr, src).wait()


def run_head(x, u_row, v_row):
    n_src, n_arr, rows, dim = x.shape
    seq = n_src * rows
    n_tiles = seq // TILE
    bf16 = jnp.bfloat16
    f32 = jnp.float32
    vmem = pl.BlockSpec(memory_space=pltpu.VMEM)
    tall = pltpu.VMEM((seq, dim), bf16)
    return pl.pallas_call(
        head_kernel,
        out_shape=(jax.ShapeDtypeStruct((n_src, 4, rows, dim), bf16), jax.ShapeDtypeStruct((seq, dim), bf16), jax.ShapeDtypeStruct((8, dim), f32)),
        in_specs=[pl.BlockSpec(memory_space=pl.ANY), vmem, vmem],
        out_specs=(pl.BlockSpec(memory_space=pl.ANY), vmem, vmem),
        scratch_shapes=[
            tall, tall, tall, tall, tall,
            pltpu.VMEM((n_tiles, TILE, TILE), f32),
            pltpu.VMEM((2, TILE, TILE), f32),
            pltpu.VMEM((2, TILE, TILE), f32),
            pltpu.VMEM((TILE, dim), f32),
            pltpu.VMEM((TILE, dim), f32),
            pltpu.VMEM((TILE, dim), f32),
            pltpu.VMEM((TILE, BLK), f32),
            pltpu.VMEM((TILE, BLK), f32),
            pltpu.VMEM((TILE, dim), bf16),
            pltpu.VMEM((TILE, dim), bf16),
            pltpu.VMEM((dim, TILE), bf16),
            pltpu.VMEM((dim, TILE), bf16),
            pltpu.VMEM((dim, TILE), bf16),
            pltpu.VMEM((n_tiles, dim, TILE), f32),
            pltpu.VMEM((n_tiles, dim, TILE), f32),
            pltpu.VMEM((n_tiles, dim, TILE), f32),
            pltpu.VMEM((4, n_src, rows, dim), bf16),
            pltpu.SemaphoreType.DMA((n_arr, n_src)),
            pltpu.SemaphoreType.DMA((n_arr, n_src)),
            pltpu.SemaphoreType.DMA((4, n_src)),
            pltpu.SemaphoreType.DMA((4, n_src)),
        ],
        compiler_params=pltpu.CompilerParams(vmem_limit_bytes=60 * 1024 * 1024, collective_id=0, has_side_effects=True),
        cost_estimate=pl.CostEstimate(flops=9 * seq * seq * dim, bytes_accessed=4 * seq * n_arr * dim, transcendentals=seq * seq // 2),
        name='rel_attention_head',
    )(x, u_row, v_row)


def solution(mesh):
    seq_spec = P('cp', 'hp', None)
    head_spec = P('hp', None)
    weight_spec = P(None, 'hp', None)

    def local_fn(q, k, v, u_bias, v_bias, rel_table, w_rel, d_out):
        block_len, num_heads, head_dim = q.shape
        model_dim = rel_table.shape[1]
        f32 = jnp.float32
        bf16 = jnp.bfloat16
        me = lax.axis_index('cp')
        table_all = lax.all_gather(rel_table, 'cp', axis=0, tiled=True)
        rel_mine = jnp.dot(rel_table, w_rel.reshape(model_dim, num_heads * head_dim), preferred_element_type=f32)
        rel_mine = rel_mine.astype(bf16).reshape(block_len, num_heads, head_dim)
        packed = jnp.stack([q, k, v, d_out, rel_mine], axis=0).transpose(2, 0, 1, 3)
        u_row = lax.dynamic_slice_in_dim(u_bias, me, 1, 0)
        v_row = lax.dynamic_slice_in_dim(v_bias, me, 1, 0)
        y, d_rel, sums = run_head(packed, u_row, v_row)
        back = y.transpose(1, 2, 0, 3)
        d_w = lax.dot_general(table_all, d_rel, (((0,), (0,)), ((), ())), preferred_element_type=f32)
        tail = lax.all_gather(jnp.concatenate([d_w, sums], axis=0), 'cp')
        d_w_rel = tail[:, :model_dim].transpose(1, 0, 2)
        return back[0], back[1], back[2], back[3], tail[:, model_dim], tail[:, model_dim + 1], d_w_rel

    return jax.shard_map(
        local_fn,
        mesh=mesh,
        in_specs=(seq_spec, seq_spec, seq_spec, head_spec, head_spec, P('cp', None), weight_spec, seq_spec),
        out_specs=(seq_spec, seq_spec, seq_spec, seq_spec, head_spec, head_spec, weight_spec),
        check_vma=False,
    )
```

```python
import functools
import jax
import jax.numpy as jnp
from jax import lax
from jax.experimental import pallas as pl
from jax.experimental.pallas import tpu as pltpu
from jax.sharding import PartitionSpec as P

TILE = 768
BLK = 128
LOG2E = 1.4426950408889634


def dot_nt(lhs, rhs):
    return lax.dot_general(lhs, rhs, (((1,), (1,)), ((), ())), preferred_element_type=jnp.float32)


def dot_nn(lhs, rhs):
    return lax.dot_general(lhs, rhs, (((1,), (0,)), ((), ())), preferred_element_type=jnp.float32)


def head_kernel(xq_hbm, xk_hbm, xv_hbm, xg_hbm, xr_hbm, table_hbm, u_ref, w_ref,
                yo_hbm, yq_hbm, yk_hbm, yv_hbm, tab_hbm, dw_hbm,
                q_s, k_s, v_s, g_s, r_s, score_s, roll_s, ds_s, out_s, gu_s, gv_s, max_s, sum_s,
                qv_s, qu_s, quT_s, qvT_s, gT_s, dk_s, dv_s, dr_s, stage_s,
                sums_ref, tbuf_s, dwT_s, dw_s,
                in_send, in_recv, out_send, out_recv, tab_send, tab_recv, dw_send, dw_recv, load_sem):
    n_src, rows, dim = xq_hbm.shape
    model_dim = table_hbm.shape[1]
    x_hbm = (xq_hbm, xk_hbm, xv_hbm, xg_hbm, xr_hbm)
    y_hbm = (yo_hbm, yq_hbm, yk_hbm, yv_hbm)
    n_tiles = n_src * rows // TILE
    nb = TILE // BLK
    inv_sqrt = dim ** -0.5
    scale2 = inv_sqrt * LOG2E
    bf16 = jnp.bfloat16
    f32 = jnp.float32

    me = lax.axis_index('cp')
    n_dev = n_src
    arrays = (q_s, k_s, v_s, g_s, r_s)

    def arrive(arr, src):
        rows_of = arrays[arr].at[pl.ds(pl.multiple_of(src * rows, rows), rows)]
        return pltpu.make_async_copy(x_hbm[arr].at[me], rows_of, in_recv.at[arr, src])

    def depart(arr, dest):
        return pltpu.make_async_remote_copy(
            src_ref=x_hbm[arr].at[dest],
            dst_ref=arrays[arr].at[pl.ds(pl.multiple_of(me * rows, rows), rows)],
            send_sem=in_send.at[arr, dest], recv_sem=in_recv.at[arr, me],
            device_id={'cp': dest}, device_id_type=pl.DeviceIdType.MESH)

    def give(arr, dest):
        return pltpu.make_async_remote_copy(
            src_ref=stage_s.at[arr, dest], dst_ref=y_hbm[arr].at[me],
            send_sem=out_send.at[arr, dest], recv_sem=out_recv.at[arr, me],
            device_id={'cp': dest}, device_id_type=pl.DeviceIdType.MESH)

    def keep(arr, src):
        return pltpu.make_async_copy(stage_s.at[arr, me], y_hbm[arr].at[src], out_recv.at[arr, src])

    def hand_out(arr, dest):
        @pl.when(dest != me)
        def _():
            give(arr, dest).start()

        @pl.when(dest == me)
        def _():
            keep(arr, me).start()

    core = lax.rem(me, 2)
    chip = me // 2
    partner = 2 * chip + 1 - core
    peers = [2 * lax.rem(chip + step, n_dev // 2) + core for step in range(1, n_dev // 2)]
    cousins = [2 * lax.rem(chip + step, n_dev // 2) + 1 - core for step in range(1, n_dev // 2)]

    def send_table(slot, src_ref, owner, dest):
        return pltpu.make_async_remote_copy(
            src_ref=src_ref, dst_ref=tab_hbm.at[owner],
            send_sem=tab_send.at[slot], recv_sem=tab_recv.at[owner],
            device_id={'cp': dest}, device_id_type=pl.DeviceIdType.MESH)

    def table_here(owner):
        return pltpu.make_async_copy(table_hbm, tab_hbm.at[owner], tab_recv.at[owner])

    def send_dw(slot, src_ref, owner, dest):
        return pltpu.make_async_remote_copy(
            src_ref=src_ref, dst_ref=dw_hbm.at[owner],
            send_sem=dw_send.at[slot], recv_sem=dw_recv.at[owner],
            device_id={'cp': dest}, device_id_type=pl.DeviceIdType.MESH)

    def dw_here(owner):
        return pltpu.make_async_copy(dw_s, dw_hbm.at[owner], dw_recv.at[owner])

    def load_table(m, slot):
        return pltpu.make_async_copy(tab_hbm.at[m], tbuf_s.at[slot], load_sem.at[slot])

    def start_load(m, slot):
        @pl.when(m != me)
        def _():
            load_table(m, slot).start()

        @pl.when(m == me)
        def _():
            pltpu.make_async_copy(table_hbm, tbuf_s.at[slot], load_sem.at[slot]).start()

    barrier = pltpu.get_barrier_semaphore()
    for step in range(1, n_dev):
        pl.semaphore_signal(barrier, inc=1, device_id={'cp': lax.rem(me + step, n_dev)}, device_id_type=pl.DeviceIdType.MESH)
    pl.semaphore_wait(barrier, n_dev - 1)
    order = (1, 0, 4, 2, 3)
    for arr in order:
        for step in range(1, n_dev):
            depart(arr, lax.rem(me + step, n_dev)).start()
        arrive(arr, me).start()
    direct = peers + [partner]
    for slot, dest in enumerate(direct):
        send_table(slot, table_hbm, me, dest).start()

    sums_ref[...] = jnp.zeros_like(sums_ref)
    dk_s[...] = jnp.zeros_like(dk_s)
    dv_s[...] = jnp.zeros_like(dv_s)
    dr_s[...] = jnp.zeros_like(dr_s)

    row_id = lax.broadcasted_iota(jnp.int32, (BLK, BLK), 0)
    col_id = lax.broadcasted_iota(jnp.int32, (BLK, BLK), 1)
    low = col_id <= row_id

    def tile_rows(ref, idx):
        return ref[pl.ds(pl.multiple_of(idx * TILE, TILE), TILE), :]

    def blk(ref, slot, h, u):
        return ref[slot, pl.ds(h * BLK, BLK), pl.ds(u * BLK, BLK)]

    def by_off(ref, cur, prev, h, d):
        return blk(ref, cur, h, d) if d >= 0 else blk(ref, prev, h, d + nb)

    flip = jnp.where(row_id + col_id == BLK - 1, 1.0, 0.0).astype(bf16)

    back_idx = lax.rem(col_id + row_id + 1, BLK)

    def unroll_blk(x):
        return jnp.take_along_axis(x, back_idx, axis=1)

    @pl.loop(0, n_tiles)
    def _(i):
        @pl.when(i == n_tiles - 2)
        def _():
            for slot, owner in enumerate(peers):
                table_here(owner).wait()
                send_table(len(direct) + slot, tab_hbm.at[owner], owner, partner).start()

        for arr in order[:3]:
            arrive(arr, i).wait()
        for b in range(nb):
            here = pl.ds(pl.multiple_of(i * TILE + b * BLK, BLK), BLK)
            r_s[here, :] = dot_nn(flip, r_s[here, :]).astype(bf16)
        q_wide = tile_rows(q_s, i).astype(f32)
        qu_f = q_wide + u_ref[...]
        qv_f = q_wide + w_ref[...]
        qu_s[...] = qu_f.astype(bf16)
        qv_s[...] = qv_f.astype(bf16)
        quT_s[...] = qu_f.T.astype(bf16)
        qvT_s[...] = qv_f.T.astype(bf16)
        max_s[...] = jnp.full_like(max_s, -jnp.inf)
        sum_s[...] = jnp.zeros_like(sum_s)
        out_s[...] = jnp.zeros_like(out_s)
        gu_s[...] = jnp.zeros_like(gu_s)
        gv_s[...] = jnp.zeros_like(gv_s)

        def score_step(m, diag):
            kt = i - m
            cur = lax.rem(m, 2)
            prev = 1 - cur
            by_offset = dot_nt(qv_s[...], tile_rows(r_s, m))
            for h in range(nb):
                for d in range(nb):
                    piece = by_offset[h * BLK:(h + 1) * BLK, d * BLK:(d + 1) * BLK]
                    roll_s[cur, pl.ds(h * BLK, BLK), pl.ds(d * BLK, BLK)] = pltpu.roll(piece, 1, 1, stride=1, stride_axis=0)
            content = dot_nt(qu_s[...], tile_rows(k_s, kt))
            for h in range(nb):
                top = max_s[pl.ds(h * BLK, BLK), :]
                for u in range(nb):
                    piece = content[h * BLK:(h + 1) * BLK, u * BLK:(u + 1) * BLK]
                    if diag and u > h:
                        s_blk = jnp.full((BLK, BLK), -jnp.inf, f32)
                    elif diag and u == h:
                        s_blk = jnp.where(low, piece + by_off(roll_s, cur, prev, h, 0), -jnp.inf)
                    else:
                        s_blk = piece + jnp.where(low, by_off(roll_s, cur, prev, h, h - u), by_off(roll_s, cur, prev, h, h - u - 1))
                    score_s[kt, pl.ds(h * BLK, BLK), pl.ds(u * BLK, BLK)] = s_blk
                    top = jnp.maximum(top, s_blk)
                max_s[pl.ds(h * BLK, BLK), :] = top

        score_step(0, True)

        @pl.loop(1, i + 1)
        def _(m):
            score_step(m, False)

        arrive(2, i).wait()
        row_max = jnp.max(max_s[...], axis=1, keepdims=True) * scale2

        @pl.loop(0, i + 1)
        def _(kt):
            prob = jnp.exp2(score_s[kt] * scale2 - row_max)
            score_s[kt] = prob
            part = prob[:, :BLK]
            for u in range(1, nb):
                part = part + prob[:, u * BLK:(u + 1) * BLK]
            sum_s[...] += part
            out_s[...] += dot_nn(prob.astype(bf16), tile_rows(v_s, kt))

        arrive(3, i).wait()
        g_tile = tile_rows(g_s, i)
        gT_s[...] = g_tile.astype(f32).T.astype(bf16)
        inv_sum = 1.0 / jnp.sum(sum_s[...], axis=1, keepdims=True)
        out = out_s[...] * inv_sum
        delta = jnp.sum(out * g_tile.astype(f32), axis=1, keepdims=True)
        stage_s[0, i] = out.astype(bf16)

        @pl.when(i > 0)
        def _():
            hand_out(1, i - 1)

        @pl.when(i == n_tiles - 1)
        def _():
            for owner in [partner] + cousins:
                table_here(owner).wait()
            start_load(n_tiles - 1, 0)
            dwT_s[...] = jnp.zeros_like(dwT_s)

        ds_s[1] = jnp.zeros((TILE, TILE), f32)

        @pl.loop(0, i + 1)
        def _(kt):
            m = i - kt
            cur = lax.rem(kt, 2)
            prev = 1 - cur
            d_prob = dot_nt(tile_rows(g_s, i), tile_rows(v_s, kt))
            prob = score_s[kt] * inv_sum
            d_score = prob * (d_prob - delta)
            ds_s[cur] = d_score
            prob_b = prob.astype(bf16)
            ds_b = d_score.astype(bf16)
            dv_s[kt] += dot_nn(gT_s[...], prob_b)
            dk_s[kt] += dot_nn(quT_s[...], ds_b)
            gu_s[...] += dot_nn(ds_b, tile_rows(k_s, kt))
            out_rows = []
            for h in range(nb):
                cols = []
                for d in range(nb):
                    near = by_off(ds_s, cur, prev, h, h - d)
                    far = by_off(ds_s, cur, prev, h, h - d - 1)
                    cols.append(unroll_blk(jnp.where(low, near, far)))
                out_rows.append(jnp.concatenate(cols, axis=1))
            wide = jnp.concatenate(out_rows, axis=0).astype(bf16)
            gv_s[...] += dot_nn(wide, tile_rows(r_s, m))
            dr_s[m] += dot_nn(qvT_s[...], wide)

            @pl.when(i == n_tiles - 1)
            def _():
                slot = lax.rem(kt, 2)

                @pl.when(m > 0)
                def _():
                    start_load(m - 1, 1 - slot)

                d_rel = (dr_s[m] * inv_sqrt).astype(bf16)
                d_rel = [dot_nn(d_rel[:, b * BLK:(b + 1) * BLK], flip).astype(bf16) for b in range(nb)]
                load_table(m, slot).wait()
                dwT_s[...] += dot_nn(jnp.concatenate(d_rel, axis=1), tbuf_s[slot])
                stage_s[2, kt] = (dk_s[kt] * inv_sqrt).T.astype(bf16)
                stage_s[3, kt] = dv_s[kt].T.astype(bf16)

                @pl.when(kt > 0)
                def _():
                    hand_out(2, kt - 1)
                    hand_out(3, kt - 1)

        hand_out(0, i)
        gu = gu_s[...] * inv_sqrt
        gv = gv_s[...] * inv_sqrt
        stage_s[1, i] = (gu + gv).astype(bf16)
        sums_ref[0:1, :] += jnp.sum(gu, axis=0, keepdims=True)
        sums_ref[1:2, :] += jnp.sum(gv, axis=0, keepdims=True)

    hand_out(2, n_tiles - 1)
    hand_out(3, n_tiles - 1)
    dw_s[0:model_dim, :] = dwT_s[...].T
    dw_s[model_dim:, :] = sums_ref[...]
    hand_out(1, n_tiles - 1)
    for slot, dest in enumerate(direct):
        send_dw(slot, dw_s, me, dest).start()
    dw_here(me).start()
    for step in range(1, n_dev):
        dest = lax.rem(me + step, n_dev)
        for arr in range(5):
            depart(arr, dest).wait_send()
        for arr in range(4):
            give(arr, dest).wait_send()
    for slot, owner in enumerate(peers):
        dw_here(owner).wait()
        send_dw(len(direct) + slot, dw_hbm.at[owner], owner, partner).start()
    for src in range(n_dev):
        for arr in range(4):
            keep(arr, src).wait()
    for slot in range(2 * len(direct) - 1):
        send_table(slot, table_hbm, me, partner).wait_send()
        send_dw(slot, dw_s, me, partner).wait_send()
    for owner in [me, partner] + cousins:
        dw_here(owner).wait()


def run_head(xs, table, u_row, v_row):
    n_src, rows, dim = xs[0].shape
    n_arr = len(xs)
    model_dim = table.shape[1]
    seq = n_src * rows
    n_tiles = seq // TILE
    bf16 = jnp.bfloat16
    f32 = jnp.float32
    vmem = pl.BlockSpec(memory_space=pltpu.VMEM)
    anywhere = pl.BlockSpec(memory_space=pl.ANY)
    tall = pltpu.VMEM((seq, dim), bf16)
    return pl.pallas_call(
        head_kernel,
        out_shape=tuple([jax.ShapeDtypeStruct((n_src, rows, dim), bf16)] * 4) + (
            jax.ShapeDtypeStruct((n_src, rows, model_dim), bf16),
            jax.ShapeDtypeStruct((n_src, model_dim + 8, dim), f32),
        ),
        in_specs=[anywhere] * 6 + [vmem, vmem],
        out_specs=(anywhere,) * 6,
        scratch_shapes=[
            tall, tall, tall, tall, tall,
            pltpu.VMEM((n_tiles, TILE, TILE), f32),
            pltpu.VMEM((2, TILE, TILE), f32),
            pltpu.VMEM((2, TILE, TILE), f32),
            pltpu.VMEM((TILE, dim), f32),
            pltpu.VMEM((TILE, dim), f32),
            pltpu.VMEM((TILE, dim), f32),
            pltpu.VMEM((TILE, BLK), f32),
            pltpu.VMEM((TILE, BLK), f32),
            pltpu.VMEM((TILE, dim), bf16),
            pltpu.VMEM((TILE, dim), bf16),
            pltpu.VMEM((dim, TILE), bf16),
            pltpu.VMEM((dim, TILE), bf16),
            pltpu.VMEM((dim, TILE), bf16),
            pltpu.VMEM((n_tiles, dim, TILE), f32),
            pltpu.VMEM((n_tiles, dim, TILE), f32),
            pltpu.VMEM((n_tiles, dim, TILE), f32),
            pltpu.VMEM((4, n_src, rows, dim), bf16),
            pltpu.VMEM((8, dim), f32),
            pltpu.VMEM((2, rows, model_dim), bf16),
            pltpu.VMEM((dim, model_dim), f32),
            pltpu.VMEM((model_dim + 8, dim), f32),
            pltpu.SemaphoreType.DMA((n_arr, n_src)),
            pltpu.SemaphoreType.DMA((n_arr, n_src)),
            pltpu.SemaphoreType.DMA((4, n_src)),
            pltpu.SemaphoreType.DMA((4, n_src)),
            pltpu.SemaphoreType.DMA((n_src - 1,)),
            pltpu.SemaphoreType.DMA((n_src,)),
            pltpu.SemaphoreType.DMA((n_src - 1,)),
            pltpu.SemaphoreType.DMA((n_src,)),
            pltpu.SemaphoreType.DMA((2,)),
        ],
        compiler_params=pltpu.CompilerParams(vmem_limit_bytes=66 * 1000 * 1000, collective_id=0, has_side_effects=True),
        cost_estimate=pl.CostEstimate(flops=9 * seq * seq * dim, bytes_accessed=4 * seq * n_arr * dim, transcendentals=seq * seq // 2),
        name='rel_attention_head',
    )(*xs, table, u_row, v_row)


def solution(mesh):
    seq_spec = P('cp', 'hp', None)
    head_spec = P('hp', None)
    weight_spec = P(None, 'hp', None)

    def local_fn(q, k, v, u_bias, v_bias, rel_table, w_rel, d_out):
        block_len, num_heads, head_dim = q.shape
        model_dim = rel_table.shape[1]
        f32 = jnp.float32
        bf16 = jnp.bfloat16
        me = lax.axis_index('cp')
        rel_mine = jnp.dot(rel_table, w_rel.reshape(model_dim, num_heads * head_dim), preferred_element_type=f32)
        rel_mine = rel_mine.astype(bf16).reshape(block_len, num_heads, head_dim)
        xs = [arr.transpose(1, 0, 2) for arr in (q, k, v, d_out, rel_mine)]
        u_row = lax.dynamic_slice_in_dim(u_bias, me, 1, 0)
        v_row = lax.dynamic_slice_in_dim(v_bias, me, 1, 0)
        *ys, _, tail = run_head(xs, rel_table, u_row, v_row)
        outs = [y.transpose(1, 0, 2) for y in ys]
        return (*outs, tail[:, model_dim], tail[:, model_dim + 1], tail[:, :model_dim].transpose(1, 0, 2))

    return jax.shard_map(
        local_fn,
        mesh=mesh,
        in_specs=(seq_spec, seq_spec, seq_spec, head_spec, head_spec, P('cp', None), weight_spec, seq_spec),
        out_specs=(seq_spec, seq_spec, seq_spec, seq_spec, head_spec, head_spec, weight_spec),
        check_vma=False,
    )
```
